32 devices in a mesh: patch: 8 (over y, x, core), tensor: 4 (over z).
Axes of the slice: x: 2, y: 2, z: 4, core: 2. Of those that a mesh axis runs over, the one named last changes fastest.
Arguments:
- tokens: bfloat16 [8192, 3072], P(('patch', 'tensor')), may hold values from -6 to 6
- text_tokens: bfloat16 [512, 3072], P('patch'), may hold values from -6 to 6
- img_shift: float32 [3072], replicated, may hold values from -3 to 3
- img_scale: float32 [3072], replicated, may hold values from -3 to 3
- img_gate: float32 [3072], replicated, may hold values from 0.5 to 2
- txt_shift: float32 [3072], replicated, may hold values from -3 to 3
- txt_scale: float32 [3072], replicated, may hold values from -3 to 3
- qkv_weight: bfloat16 [3072, 3, 2048], P(None, None, 'tensor'), may hold values from -0.109375 to 0.109375
- txt_kv_weight: bfloat16 [3072, 2, 2048], P(None, None, 'tensor'), may hold values from -0.109375 to 0.109375
- q_gain: float32 [128], replicated, may hold values from 1 to 3
- k_gain: float32 [128], replicated, may hold values from 1 to 3
- txt_k_gain: float32 [128], replicated, may hold values from 1 to 3
- out_weight: bfloat16 [2048, 3072], P('tensor'), may hold values from -0.125 to 0.125
- stale_keys: bfloat16 [8192, 2048], P('patch', 'tensor'), may hold values from -600 to 600
- stale_values: bfloat16 [8192, 2048], P('patch', 'tensor'), may hold values from -6 to 6
Outputs:
- updated: bfloat16 [8192, 3072], P(('patch', 'tensor'))
- new_keys: bfloat16 [8192, 2048], P('patch', 'tensor')
- new_values: bfloat16 [8192, 2048], P('patch', 'tensor')
The draws below stay inside these ranges and needn't reach their ends.
All inputs are finite; a program needn't handle non-finite values.
Results may differ from the reference program's by a relative error of at most 0.015.
The reference program's roundings to bfloat16 on the way (of `image_mod`, `text_mod` and `attended`) count: a program that leaves them out, or rounds other values in their place, can miss the bound.
Values may be sent and summed in bfloat16 or wider, within the bound.
A program may use at most 320 MiB of HBM per device.

```python
import math
import jax
import jax.numpy as jnp
from jax import lax

D = 3072
HD = 128
HEADS = 16
ROWS = 1024
TXT = 512
IMG = 8192
N_PATCH = 8


def draw_stale_keys(key, part):
    first = jax.random.fold_in(key, 0)
    base = jnp.clip(2.0 * jax.random.normal(first, (IMG, HEADS * HD), jnp.float32), -12.0, 12.0)
    return base.astype(jnp.bfloat16)


def block_levels(rng, dims, shards, smallest, high):
    def one(dim, blocks):
        steps = jax.random.uniform(jax.random.fold_in(jax.random.fold_in(rng, 6), dim), (blocks,), jnp.float32, smallest / len(shards), high / len(shards))
        return jnp.repeat(jnp.exp(steps), dims[dim] // blocks).reshape((-1,) + (1,) * (len(dims) - dim - 1))

    loudness = one(*shards[0])
    for cut in shards[1:]:
        loudness = loudness * one(*cut)
    return loudness


def scatter_about(rng, shape, deviation, reach, cuts=(), kind=jnp.bfloat16):
    level = block_levels(rng, shape, cuts, -0.22, 0.18) if cuts else 1.0
    result = jax.random.normal(rng, shape, jnp.float32) * deviation * level
    return jnp.minimum(jnp.maximum(result, -reach), reach).astype(kind)


def setup_inputs(seed: int = 0) -> dict:
    keys = jax.random.split(jax.random.key(seed), 16)
    tokens = scatter_about(keys[0], (IMG, D), 1.0, 6.0, ((0, 32),))
    text_tokens = scatter_about(keys[1], (TXT, D), 1.0, 6.0, ((0, 8),))
    img_shift = scatter_about(keys[2], (D,), 0.5, 3.0, (), jnp.float32)
    img_scale = scatter_about(keys[3], (D,), 0.5, 3.0, (), jnp.float32)
    img_gate = jnp.clip(jax.random.uniform(keys[4], (D,), jnp.float32, 0.5, 2.0), 0.5, 2.0)
    txt_shift = scatter_about(keys[5], (D,), 0.5, 3.0, (), jnp.float32)
    txt_scale = scatter_about(keys[6], (D,), 0.5, 3.0, (), jnp.float32)
    qkv_weight = scatter_about(keys[7], (D, 3, HEADS * HD), D ** -0.5, 0.109375, ((2, 4),))
    txt_kv_weight = scatter_about(keys[8], (D, 2, HEADS * HD), D ** -0.5, 0.109375, ((2, 4),))
    q_gain = jnp.clip(jnp.exp(jax.random.uniform(keys[9], (HD,), jnp.float32, math.log(1.0), math.log(3.0))), 1.0, 3.0)
    k_gain = jnp.clip(jnp.exp(jax.random.uniform(keys[10], (HD,), jnp.float32, math.log(1.0), math.log(3.0))), 1.0, 3.0)
    txt_k_gain = jnp.clip(jnp.exp(jax.random.uniform(keys[11], (HD,), jnp.float32, math.log(1.0), math.log(3.0))), 1.0, 3.0)
    out_weight = scatter_about(keys[12], (HEADS * HD, D), (HEADS * HD) ** -0.5, 0.125, ((0, 4),))
    stale_keys = draw_stale_keys(jax.random.fold_in(keys[15], 71), 0)
    stale_values = scatter_about(keys[14], (IMG, HEADS * HD), 1.0, 6.0, ((0, 8), (1, 4)))
    return dict(tokens=tokens, text_tokens=text_tokens, img_shift=img_shift, img_scale=img_scale, img_gate=img_gate, txt_shift=txt_shift, txt_scale=txt_scale, qkv_weight=qkv_weight, txt_kv_weight=txt_kv_weight, q_gain=q_gain, k_gain=k_gain, txt_k_gain=txt_k_gain, out_weight=out_weight, stale_keys=stale_keys, stale_values=stale_values)


def layer_mod(values, shift_vec, scale_vec):
    wide = values.astype(jnp.float32)
    centre = lax.optimization_barrier(jnp.mean(wide, axis=-1, keepdims=True))
    spread = lax.optimization_barrier(jnp.mean((wide - centre) * (wide - centre), axis=-1, keepdims=True))
    normed = (wide - centre) * lax.rsqrt(spread + 1e-06)
    return ((1.0 + scale_vec) * normed + shift_vec).astype(jnp.bfloat16)

def rms_gain(values, gain_vec):
    square = lax.optimization_barrier(jnp.mean(values * values, axis=-1, keepdims=True))
    return values * lax.rsqrt(square + 1e-06) * gain_vec

def reference(tokens, text_tokens, img_shift, img_scale, img_gate, txt_shift, txt_scale, qkv_weight, txt_kv_weight, q_gain, k_gain, txt_k_gain, out_weight, stale_keys, stale_values):
    image_mod = layer_mod(tokens, img_shift, img_scale)
    projected = jnp.dot(image_mod, qkv_weight.reshape(D, 3 * HEADS * HD), preferred_element_type=jnp.float32)
    projected = projected.reshape(IMG, 3, HEADS, HD)
    queries = rms_gain(projected[:, 0], q_gain).astype(jnp.bfloat16)
    fresh_keys = rms_gain(projected[:, 1], k_gain).astype(jnp.bfloat16)
    fresh_values = projected[:, 2].astype(jnp.bfloat16)
    text_mod = layer_mod(text_tokens, txt_shift, txt_scale)
    text_proj = jnp.dot(text_mod, txt_kv_weight.reshape(D, 2 * HEADS * HD), preferred_element_type=jnp.float32)
    text_proj = text_proj.reshape(TXT, 2, HEADS, HD)
    text_keys = rms_gain(text_proj[:, 0], txt_k_gain).astype(jnp.bfloat16)
    text_values = text_proj[:, 1].astype(jnp.bfloat16)
    old_keys = stale_keys.reshape(IMG, HEADS, HD)
    old_values = stale_values.reshape(IMG, HEADS, HD)
    factor = 1.0 / math_sqrt(HD)
    zero = jnp.int32(0)

    def one_patch(patch_idx):
        offset = (patch_idx * ROWS).astype(jnp.int32)
        own_keys = lax.dynamic_slice_in_dim(fresh_keys, offset, ROWS, 0)
        own_values = lax.dynamic_slice_in_dim(fresh_values, offset, ROWS, 0)
        key_rows = lax.dynamic_update_slice(old_keys, own_keys, (offset, zero, zero))
        value_rows = lax.dynamic_update_slice(old_values, own_values, (offset, zero, zero))
        key_rows = jnp.concatenate([key_rows, text_keys], axis=0)
        value_rows = jnp.concatenate([value_rows, text_values], axis=0)
        query_rows = lax.dynamic_slice_in_dim(queries, offset, ROWS, 0)
        scores = jnp.einsum('qhd,khd->hqk', query_rows.astype(jnp.float32), key_rows.astype(jnp.float32)) * factor
        highest = lax.optimization_barrier(jnp.max(scores, axis=-1, keepdims=True))
        weights = jnp.exp(scores - highest)
        denominator = lax.optimization_barrier(jnp.sum(weights, axis=-1))
        rounded = weights.astype(jnp.bfloat16).astype(jnp.float32)
        numerator = jnp.einsum('hqk,khd->qhd', rounded, value_rows.astype(jnp.float32))
        return (numerator / jnp.transpose(denominator)[:, :, None]).astype(jnp.bfloat16)
    attended = lax.map(one_patch, jnp.arange(N_PATCH, dtype=jnp.int32)).reshape(IMG, HEADS * HD)
    branch = jnp.dot(attended, out_weight, preferred_element_type=jnp.float32)
    updated = (tokens.astype(jnp.float32) + img_gate * branch).astype(jnp.bfloat16)
    return (updated, fresh_keys.reshape(IMG, HEADS * HD), fresh_values.reshape(IMG, HEADS * HD))

def math_sqrt(number):
    return float(number) ** 0.5
```

```python
import functools
import math

import jax
import jax.numpy as jnp
from jax import lax
from jax.experimental import pallas as pl
from jax.experimental.pallas import tpu as pltpu
from jax.sharding import PartitionSpec as P

MESH = pl.DeviceIdType.MESH
ANY = pl.BlockSpec(memory_space=pl.ANY)
VMEM = pl.BlockSpec(memory_space=pltpu.VMEM)


def layer_mod(values, shift_vec, scale_vec):
    wide = values.astype(jnp.float32)
    centre = jnp.mean(wide, axis=-1, keepdims=True)
    off = wide - centre
    spread = jnp.mean(off * off, axis=-1, keepdims=True)
    return ((1.0 + scale_vec) * (off * lax.rsqrt(spread + 1e-06)) + shift_vec).astype(jnp.bfloat16)


def mod_kernel(x_ref, shift_ref, scale_ref, o_ref):
    o_ref[...] = layer_mod(x_ref[...], shift_ref[...], scale_ref[...])


def modulate(x, shift, scale):
    rows, width = x.shape
    tile = min(rows, 64)
    return pl.pallas_call(
        mod_kernel,
        grid=(rows // tile,),
        out_shape=jax.ShapeDtypeStruct((rows, width), jnp.bfloat16),
        in_specs=[
            pl.BlockSpec((tile, width), lambda i: (i, 0)),
            pl.BlockSpec((1, width), lambda i: (0, 0)),
            pl.BlockSpec((1, width), lambda i: (0, 0)),
        ],
        out_specs=pl.BlockSpec((tile, width), lambda i: (i, 0)),
        name="modulate",
    )(x, shift[None, :], scale[None, :])


def rms_gain(piece, gain):
    square = jnp.mean(piece * piece, axis=-1, keepdims=True)
    return piece * lax.rsqrt(square + 1e-06) * gain


def fused_kernel(
    n_p, n_t, scale,
    x_ref, text_ref, tshift_ref, tscale_ref, w_hbm, wt_hbm, qg_ref, kg_ref, tg_ref, ow_ref, sk_ref, sv_ref,
    nk_ref, nv_ref, att_ref, wall_ref,
    xall, w, wt, kall, vall, tk, tv, q_ref, m_ref, l_ref, acc_ref, asend,
    load_sem, kv_send, kv_recv, z_send, z_recv, tx_send, tx_recv, w_send, w_recv, a_send, a_recv, out_sem,
):
    me = lax.axis_index("patch")
    t = lax.axis_index("tensor")
    rows, width = x_ref.shape
    keys, cols = sk_ref.shape
    hd = qg_ref.shape[1]
    heads = cols // hd
    half = keys // 2
    hrows = rows // 2
    trows = text_ref.shape[0]
    share = ow_ref.shape[0] // n_p
    wcols = width // 2
    bits = n_p.bit_length() - 1
    orders = (list(range(1, bits)), list(range(1, bits))[::-1])
    last_rank = 1 << (bits - 1)

    def unrank(h, r):
        return sum(1 << b for pos, b in enumerate(orders[h]) if r >> pos & 1)

    def owner(k):
        lo, hi = t, n_t - 1 - t
        near = jnp.minimum(lo, hi)
        step = lax.div(k + 1, 2)
        both = jnp.where(lax.rem(k, 2) == 1, t - step, t + step)
        one = jnp.where(lo <= hi, t + (k - near), t - (k - near))
        return jnp.where(k <= 2 * near, both, one)

    bar = pltpu.get_barrier_semaphore()

    def greet_patch(i, c):
        pl.semaphore_signal(bar, inc=1, device_id=(jnp.bitwise_xor(me, i), t), device_id_type=MESH)
        return c

    def greet_tensor(i, c):
        pl.semaphore_signal(bar, inc=1, device_id=(me, lax.rem(t + i, n_t)), device_id_type=MESH)
        return c

    lax.fori_loop(1, n_p, greet_patch, 0)
    lax.fori_loop(1, n_t, greet_tensor, 0)
    pl.semaphore_wait(bar, n_p + n_t - 2)

    def z_views(o, piece):
        if piece < 2:
            ref = xall.at[o, pl.ds(piece * hrows, hrows)]
        else:
            ref = wall_ref.at[o, me]
        return ref

    def z_copy(sgn, o, piece, first=False):
        dst = z_views(o, piece)
        src = dst
        if first:
            if piece < 2:
                src = x_ref.at[pl.ds(piece * hrows, hrows)]
            else:
                src = ow_ref.at[pl.ds(pl.multiple_of(me * share, share), share)]
        d = (sgn + 1) // 2
        return pltpu.make_async_remote_copy(
            src_ref=src, dst_ref=dst, send_sem=z_send.at[d, o, piece], recv_sem=z_recv.at[o, piece],
            device_id=(me, t + sgn), device_id_type=MESH,
        )

    def inside(i):
        return (i >= 0) & (i < n_t)

    def z_start():
        for piece in range(3):
            for sgn in (-1, 1):
                @pl.when(inside(t + sgn))
                def _():
                    z_copy(sgn, t, piece, True).start()

    def z_event(d, piece):
        for sgn in (1, -1):
            o = t - sgn * d

            @pl.when(inside(o))
            def _():
                z_copy(-sgn, o, piece).wait_recv()

                @pl.when(inside(t + sgn))
                def _():
                    z_copy(sgn, o, piece).start()

    def z_drain():
        for piece in range(3):
            for sgn in (1, -1):
                for d in range(n_t - 1):
                    o = t - sgn * d

                    @pl.when(inside(o) & inside(t + sgn))
                    def _():
                        z_copy(sgn, o, piece, d == 0).wait_send()

    def kv_copies(h, m, bit):
        slot = jnp.bitwise_xor(me, m)
        got = m ^ (1 << bit)
        out = []
        for i, (stale, every) in enumerate(((sk_ref, kall), (sv_ref, vall))):
            dst = every.at[slot, pl.ds(h * half, half)]
            src = stale.at[pl.ds(h * half, half)] if m == 0 else dst
            out.append(pltpu.make_async_remote_copy(
                src_ref=src, dst_ref=dst, send_sem=kv_send.at[h, got, i], recv_sem=kv_recv.at[h, got, i],
                device_id=(jnp.bitwise_xor(me, 1 << bit), t), device_id_type=MESH,
            ))
        return out

    def kv_wait(h, m):
        slot = jnp.bitwise_xor(me, m)
        for i, every in enumerate((kall, vall)):
            dst = every.at[slot, pl.ds(h * half, half)]
            pltpu.make_async_remote_copy(
                src_ref=dst, dst_ref=dst, send_sem=kv_send.at[h, m, i], recv_sem=kv_recv.at[h, m, i],
                device_id=(jnp.bitwise_xor(me, 1), t), device_id_type=MESH,
            ).wait_recv()

    def w_copy(k, h, m, bit):
        o = owner(k)
        got = m ^ (1 << bit)
        view = wall_ref.at[o, jnp.bitwise_xor(me, m), :, pl.ds(h * wcols, wcols)]
        return pltpu.make_async_remote_copy(
            src_ref=view, dst_ref=view, send_sem=w_send.at[k, h, got], recv_sem=w_recv.at[k, h, got],
            device_id=(jnp.bitwise_xor(me, 1 << bit), t), device_id_type=MESH,
        )

    def w_wait(k, h, m):
        o = owner(k)
        view = wall_ref.at[o, jnp.bitwise_xor(me, m), :, pl.ds(h * wcols, wcols)]
        pltpu.make_async_remote_copy(
            src_ref=view, dst_ref=view, send_sem=w_send.at[k, h, m], recv_sem=w_recv.at[k, h, m],
            device_id=(jnp.bitwise_xor(me, 1), t), device_id_type=MESH,
        ).wait_recv()

    def fan_out(h, r):
        top = r.bit_length()
        return orders[h][top:] + [0]

    def kv_event(r):
        for h in (0, 1):
            m = unrank(h, r)
            if r:
                kv_wait(h, m)
            for bit in fan_out(h, r):
                for copy in kv_copies(h, m, bit):
                    copy.start()

    def w_event(k, r):
        for h in (0, 1):
            m = unrank(h, r)
            if r:
                w_wait(k, h, m)
            for bit in fan_out(h, r):
                w_copy(k, h, m, bit).start()

    def core_wait(r):
        for h in (0, 1):
            kv_wait(h, unrank(h, r) ^ 1)

    def text_copies(i, act):
        peer = jnp.bitwise_xor(me, i)
        for j, ref in enumerate((tk, tv)):
            src = ref.at[pl.ds(pl.multiple_of(me * trows, trows), trows)]
            dst = ref.at[pl.ds(pl.multiple_of(me * trows, trows), trows)]
            act(pltpu.make_async_remote_copy(
                src_ref=src, dst_ref=dst, send_sem=tx_send.at[i, j], recv_sem=tx_recv.at[i, j],
                device_id=(peer, t), device_id_type=MESH,
            ))

    def text_wait(i):
        peer = jnp.bitwise_xor(me, i)
        for j, ref in enumerate((tk, tv)):
            dst = ref.at[pl.ds(pl.multiple_of(peer * trows, trows), trows)]
            pltpu.make_async_remote_copy(
                src_ref=dst, dst_ref=dst, send_sem=tx_send.at[i, j], recv_sem=tx_recv.at[i, j],
                device_id=(peer, t), device_id_type=MESH,
            ).wait_recv()

    def a_copy(o):
        return pltpu.make_async_remote_copy(
            src_ref=asend.at[o], dst_ref=att_ref.at[t], send_sem=a_send.at[o], recv_sem=a_recv.at[t],
            device_id=(me, o), device_id_type=MESH,
        )

    def a_wait(o):
        pltpu.make_async_remote_copy(
            src_ref=asend.at[o], dst_ref=att_ref.at[o], send_sem=a_send.at[o], recv_sem=a_recv.at[o],
            device_id=(me, o), device_id_type=MESH,
        ).wait_recv()

    def qkv(k):
        o = owner(k)
        rs = pl.multiple_of(o * rows, rows)
        x = xall[o]
        for j in range(3):
            prod = jnp.dot(x, w[j], preferred_element_type=jnp.float32)
            for h in range(heads):
                c = slice(h * hd, (h + 1) * hd)
                piece = prod[:, c]
                if j == 0:
                    q_ref[pl.ds(rs, rows), c] = rms_gain(piece, qg_ref[...]).astype(jnp.bfloat16)
                elif j == 1:
                    kall[me, pl.ds(rs, rows), c] = rms_gain(piece, kg_ref[...]).astype(jnp.bfloat16)
                else:
                    vall[me, pl.ds(rs, rows), c] = piece.astype(jnp.bfloat16)

    def stale_chunks(r, only_core=False):
        out = []
        for h in (0, 1):
            m = unrank(h, r)
            for mm in ((m ^ 1,) if only_core else (m, m ^ 1)):
                slot = jnp.bitwise_xor(me, mm)
                out.append((kall.at[slot, pl.ds(h * half, half)], vall.at[slot, pl.ds(h * half, half)]))
        return out

    def fresh_chunk(k):
        rs = pl.multiple_of(owner(k) * rows, rows)
        return (kall.at[me, pl.ds(rs, rows)], vall.at[me, pl.ds(rs, rows)])

    def attend(k, chunks, first=False, final=False):
        o = owner(k)
        rs = pl.multiple_of(o * rows, rows)

        def head(h, carry):
            c = pl.ds(pl.multiple_of(h * hd, hd), hd)
            q = q_ref[pl.ds(rs, rows), c]

            def score(chunk):
                return lax.dot_general(
                    q, chunk[0][:, c], (((1,), (1,)), ((), ())), preferred_element_type=jnp.float32
                )

            if first:
                peak = jnp.full((rows, 1), -1e30, jnp.float32)
                denom = jnp.zeros((rows, hd), jnp.float32)
                numer = jnp.zeros((rows, hd), jnp.float32)
            else:
                peak = m_ref[pl.ds(rs, rows), c][:, :1]
                denom = l_ref[pl.ds(rs, rows), c]
                numer = acc_ref[pl.ds(rs, rows), c]
            ahead = score(chunks[0])
            for idx, chunk in enumerate(chunks):
                scores = ahead
                if idx + 1 < len(chunks):
                    ahead = score(chunks[idx + 1])
                new_peak = jnp.maximum(peak, jnp.max(scores, axis=-1, keepdims=True))
                rescale = jnp.exp2((peak - new_peak) * scale)
                weights = jnp.exp2((scores - new_peak) * scale)
                step = weights.shape[1]
                if step % hd:
                    part = jnp.pad(weights, ((0, 0), (0, hd - step)))
                else:
                    part = weights[:, :hd]
                    for lane in range(hd, step, hd):
                        part = part + weights[:, lane : lane + hd]
                denom = denom * rescale + part
                numer = numer * rescale + jnp.dot(
                    weights.astype(jnp.bfloat16), chunk[1][:, c], preferred_element_type=jnp.float32
                )
                peak = new_peak
            if final:
                asend[o, :, c] = (numer / jnp.sum(denom, axis=-1, keepdims=True)).astype(jnp.bfloat16)
            else:
                m_ref[pl.ds(rs, rows), c] = jnp.broadcast_to(peak, (rows, hd))
                l_ref[pl.ds(rs, rows), c] = denom
                acc_ref[pl.ds(rs, rows), c] = numer
            return carry

        lax.fori_loop(0, heads, head, 0)

    load_x = pltpu.make_async_copy(x_ref, xall.at[t], load_sem.at[0])
    load_w = pltpu.make_async_copy(w_hbm, w, load_sem.at[1])
    load_t = pltpu.make_async_copy(wt_hbm, wt, load_sem.at[2])
    z_start()
    kv_event(0)
    load_t.start()
    load_x.start()
    load_w.start()

    text_mod = layer_mod(text_ref[...], tshift_ref[...], tscale_ref[...])
    ts = pl.multiple_of(me * trows, trows)
    load_t.wait()
    for j, ref in enumerate((tk, tv)):
        prod = jnp.dot(text_mod, wt[:, j, :], preferred_element_type=jnp.float32)
        for h in range(heads):
            c = slice(h * hd, (h + 1) * hd)
            piece = prod[:, c]
            if j == 0:
                piece = rms_gain(piece, tg_ref[...])
            ref[pl.ds(ts, trows), c] = piece.astype(jnp.bfloat16)
    load_x.wait()
    load_w.wait()
    qkv(0)

    def text_start(i, carry):
        text_copies(i, lambda copy: copy.start())
        return carry

    lax.fori_loop(1, n_p, text_start, 0)

    early = n_t // 2
    for d in range(1, early):
        z_event(d, 0)
        if d == 1:
            kv_event(1)
        z_event(d, 1)
        qkv(d)
        z_event(d, 2)
        w_event(d, 0)
    for r in range(2, last_rank - 1):
        kv_event(r)
    for r in range(last_rank - 1):
        core_wait(r)

    main = stale_chunks(0, True)
    for r in range(1, last_rank - 1):
        main = main + stale_chunks(r)
    rest = stale_chunks(last_rank - 1) + [(tk, tv)]
    fresh_early = [fresh_chunk(j) for j in range(early)]

    def early_main(k, carry):
        attend(k, main + fresh_early, first=True)
        return carry

    lax.fori_loop(0, early, early_main, 0)
    z_event(early, 0)
    kv_event(last_rank - 1)
    for d in range(1, early):
        for r in range(1, last_rank):
            w_event(d, r)
    core_wait(last_rank - 1)

    def text_done(i, carry):
        text_wait(i)
        return carry

    lax.fori_loop(1, n_p, text_done, 0)

    def early_rest(k, carry):
        attend(k, rest)
        return carry

    lax.fori_loop(0, early, early_rest, 0)

    for k in range(early, n_t):
        end = k == n_t - 1
        if k > early:
            z_event(k, 0)
        z_event(k, 1)
        if not end:
            z_event(k, 2)
            w_event(k, 0)
        qkv(k)

        def older(j, carry):
            attend(j, [fresh_chunk(k)], final=end)
            if end:
                o = owner(j)

                @pl.when(o != t)
                def _():
                    a_copy(o).start()
            return carry

        lax.fori_loop(0, k, older, 0)
        if end:
            z_event(k, 2)
            w_event(k, 0)
        fresh = [fresh_chunk(j) for j in range(k + 1)]
        attend(k, main, first=True)
        if end:
            for r in range(1, last_rank):
                w_event(k, r)
        attend(k, rest + fresh, final=end)
        if not end:
            for r in range(1, last_rank):
                w_event(k, r)
    a_copy(owner(n_t - 1)).start()

    own_att = pltpu.make_async_copy(asend.at[t], att_ref.at[t], out_sem.at[0])
    put_k = pltpu.make_async_copy(kall.at[me], nk_ref, out_sem.at[1])
    put_v = pltpu.make_async_copy(vall.at[me], nv_ref, out_sem.at[2])
    for copy in (own_att, put_k, put_v):
        copy.start()

    for k in range(1, n_t):
        for r in range(last_rank):
            for h in (0, 1):
                w_wait(k, h, unrank(h, r) ^ 1)
    z_drain()
    for r in range(last_rank):
        for h in (0, 1):
            for bit in fan_out(h, r):
                for copy in kv_copies(h, unrank(h, r), bit):
                    copy.wait_send()
    for k in range(1, n_t):
        for r in range(last_rank):
            for h in (0, 1):
                for bit in fan_out(h, r):
                    w_copy(k, h, unrank(h, r), bit).wait_send()

    def text_sent(i, carry):
        text_copies(i, lambda copy: copy.wait_send())
        return carry

    lax.fori_loop(1, n_p, text_sent, 0)
    for copy in (own_att, put_k, put_v):
        copy.wait()

    def a_done(i, carry):
        o = lax.rem(t + i, n_t)
        a_copy(o).wait_send()
        a_wait(o)
        return carry

    lax.fori_loop(1, n_t, a_done, 0)


def fused(n_p, n_t, x, text, tshift, tscale, w, wt, q_gain, k_gain, t_gain, out_weight, stale_k, stale_v):
    rows, width = x.shape
    keys, cols = stale_k.shape
    hd = q_gain.shape[0]
    trows = text.shape[0]
    share = out_weight.shape[0] // n_p
    scale = math.log2(math.e) / float(hd) ** 0.5
    bf16, f32 = jnp.bfloat16, jnp.float32
    dma = pltpu.SemaphoreType.DMA
    return pl.pallas_call(
        functools.partial(fused_kernel, n_p, n_t, scale),
        out_shape=(
            jax.ShapeDtypeStruct((keys, cols), bf16),
            jax.ShapeDtypeStruct((keys, cols), bf16),
            jax.ShapeDtypeStruct((n_t, rows, cols), bf16),
            jax.ShapeDtypeStruct((n_t, n_p, share, width), bf16),
        ),
        in_specs=[ANY, VMEM, VMEM, VMEM, ANY, ANY, VMEM, VMEM, VMEM, ANY, ANY, ANY],
        out_specs=(ANY,) * 4,
        scratch_shapes=[
            pltpu.VMEM((n_t, rows, width), bf16),
            pltpu.VMEM(w.shape, bf16),
            pltpu.VMEM(wt.shape, bf16),
            pltpu.VMEM((n_p, keys, cols), bf16),
            pltpu.VMEM((n_p, keys, cols), bf16),
            pltpu.VMEM((n_p * trows, cols), bf16),
            pltpu.VMEM((n_p * trows, cols), bf16),
            pltpu.VMEM((keys, cols), bf16),
            pltpu.VMEM((keys, cols), f32),
            pltpu.VMEM((keys, cols), f32),
            pltpu.VMEM((keys, cols), f32),
            pltpu.VMEM((n_t, rows, cols), bf16),
            dma((3,)),
            dma((2, n_p, 2)),
            dma((2, n_p, 2)),
            dma((2, n_t, 3)),
            dma((n_t, 3)),
            dma((n_p, 2)),
            dma((n_p, 2)),
            dma((n_t, 2, n_p)),
            dma((n_t, 2, n_p)),
            dma((n_t,)),
            dma((n_t,)),
            dma((3,)),
        ],
        compiler_params=pltpu.CompilerParams(
            collective_id=0, has_side_effects=True, vmem_limit_bytes=63 * 1024 * 1024
        ),
        name="fused",
    )(x, text, tshift[None, :], tscale[None, :], w, wt, q_gain[None, :], k_gain[None, :], t_gain[None, :],
      out_weight, stale_k, stale_v)


def finish_kernel(x_ref, wall_ref, ow_ref, t_ref, g_ref, o_ref):
    t = lax.axis_index("tensor")
    n_t = x_ref.shape[0]
    total = jnp.dot(x_ref[t], ow_ref[...], preferred_element_type=jnp.float32)
    for j in range(1, n_t):
        o = lax.rem(t + j, n_t)
        total = total + jnp.dot(x_ref[o], wall_ref[o], preferred_element_type=jnp.float32)
    o_ref[...] = (t_ref[...].astype(jnp.float32) + g_ref[...] * total).astype(jnp.bfloat16)


def finish(att, wall, out_weight, tokens, gate):
    n_t, rows, depth = att.shape
    width = tokens.shape[1]
    tile = 512 if width % 512 == 0 else width
    return pl.pallas_call(
        finish_kernel,
        grid=(width // tile,),
        out_shape=jax.ShapeDtypeStruct(tokens.shape, jnp.bfloat16),
        in_specs=[
            pl.BlockSpec((n_t, rows, depth), lambda j: (0, 0, 0)),
            pl.BlockSpec((n_t, depth, tile), lambda j: (0, 0, j)),
            pl.BlockSpec((depth, tile), lambda j: (0, j)),
            pl.BlockSpec((rows, tile), lambda j: (0, j)),
            pl.BlockSpec((1, tile), lambda j: (0, j)),
        ],
        out_specs=pl.BlockSpec((rows, tile), lambda j: (0, j)),
        name="finish",
    )(att, wall, out_weight, tokens, gate[None, :])


def per_device(
    n_patch,
    n_tensor,
    tokens,
    text_tokens,
    img_shift,
    img_scale,
    img_gate,
    txt_shift,
    txt_scale,
    qkv_weight,
    txt_kv_weight,
    q_gain,
    k_gain,
    txt_k_gain,
    out_weight,
    stale_keys,
    stale_values,
):
    image_mod = modulate(tokens, img_shift, img_scale)
    new_keys, new_values, att, wall = fused(
        n_patch, n_tensor, image_mod, text_tokens, txt_shift, txt_scale,
        jnp.transpose(qkv_weight, (1, 0, 2)), txt_kv_weight,
        q_gain, k_gain, txt_k_gain, out_weight, stale_keys, stale_values,
    )
    wall = wall.reshape(n_tensor, -1, wall.shape[-1])
    updated = finish(att, wall, out_weight, tokens, img_gate)
    return (updated, new_keys, new_values)


def solution(mesh):
    placed = (
        P(("patch", "tensor"), None),
        P("patch", None),
        P(),
        P(),
        P(),
        P(),
        P(),
        P(None, None, "tensor"),
        P(None, None, "tensor"),
        P(),
        P(),
        P(),
        P("tensor", None),
        P("patch", "tensor"),
        P("patch", "tensor"),
    )
    return jax.shard_map(
        functools.partial(per_device, mesh.shape["patch"], mesh.shape["tensor"]),
        mesh=mesh,
        in_specs=placed,
        out_specs=(P(("patch", "tensor"), None), P("patch", "tensor"), P("patch", "tensor")),
        check_vma=False,
    )
```

```python
import functools
import math

import jax
import jax.numpy as jnp
from jax import lax
from jax.experimental import pallas as pl
from jax.experimental.pallas import tpu as pltpu
from jax.sharding import PartitionSpec as P

MESH = pl.DeviceIdType.MESH
ANY = pl.BlockSpec(memory_space=pl.ANY)
VMEM = pl.BlockSpec(memory_space=pltpu.VMEM)


def layer_mod(values, shift_vec, scale_vec):
    wide = values.astype(jnp.float32)
    centre = jnp.mean(wide, axis=-1, keepdims=True)
    off = wide - centre
    spread = jnp.mean(off * off, axis=-1, keepdims=True)
    return ((1.0 + scale_vec) * (off * lax.rsqrt(spread + 1e-06)) + shift_vec).astype(jnp.bfloat16)


def rms_gain(piece, gain):
    square = jnp.mean(piece * piece, axis=-1, keepdims=True)
    return piece * lax.rsqrt(square + 1e-06) * gain


def fused_kernel(
    n_p, n_t, scale,
    x_ref, ishift_ref, iscale_ref, text_ref, tshift_ref, tscale_ref, w_hbm, wt_hbm, qg_ref, kg_ref, tg_ref, ow_ref, sk_ref, sv_ref,
    nk_ref, nv_ref, att_ref, wall_ref,
    xall, w, wt, kall, vall, tk, tv, q_ref, m_ref, l_ref, acc_ref, asend,
    load_sem, kv_send, kv_recv, z_send, z_recv, tx_send, tx_recv, w_send, w_recv, a_send, a_recv, out_sem,
):
    me = lax.axis_index("patch")
    t = lax.axis_index("tensor")
    rows, width = x_ref.shape
    keys, cols = sk_ref.shape
    hd = qg_ref.shape[1]
    heads = cols // hd
    half = keys // 2
    hrows = rows // 2
    trows = text_ref.shape[0]
    share = ow_ref.shape[0] // n_p
    wcols = width // 2
    bits = n_p.bit_length() - 1
    orders = (list(range(1, bits)), list(range(1, bits))[::-1])
    last_rank = 1 << (bits - 1)

    def unrank(h, r):
        return sum(1 << b for pos, b in enumerate(orders[h]) if r >> pos & 1)

    def owner(k):
        lo, hi = t, n_t - 1 - t
        near = jnp.minimum(lo, hi)
        step = lax.div(k + 1, 2)
        both = jnp.where(lax.rem(k, 2) == 1, t - step, t + step)
        one = jnp.where(lo <= hi, t + (k - near), t - (k - near))
        return jnp.where(k <= 2 * near, both, one)

    bar = pltpu.get_barrier_semaphore()

    def greet_patch(i, c):
        pl.semaphore_signal(bar, inc=1, device_id=(jnp.bitwise_xor(me, i), t), device_id_type=MESH)
        return c

    def greet_tensor(i, c):
        pl.semaphore_signal(bar, inc=1, device_id=(me, lax.rem(t + i, n_t)), device_id_type=MESH)
        return c

    lax.fori_loop(1, n_p, greet_patch, 0)
    lax.fori_loop(1, n_t, greet_tensor, 0)
    pl.semaphore_wait(bar, n_p + n_t - 2)

    def z_views(o, piece):
        if piece < 2:
            ref = xall.at[o, pl.ds(piece * hrows, hrows)]
        else:
            ref = wall_ref.at[o, me]
        return ref

    def z_copy(sgn, o, piece, first=False):
        dst = z_views(o, piece)
        src = dst
        if first:
            if piece == 2:
                src = ow_ref.at[pl.ds(pl.multiple_of(me * share, share), share)]
        d = (sgn + 1) // 2
        return pltpu.make_async_remote_copy(
            src_ref=src, dst_ref=dst, send_sem=z_send.at[d, o, piece], recv_sem=z_recv.at[o, piece],
            device_id=(me, t + sgn), device_id_type=MESH,
        )

    def inside(i):
        return (i >= 0) & (i < n_t)

    def z_start(pieces):
        for piece in pieces:
            for sgn in (-1, 1):
                @pl.when(inside(t + sgn))
                def _():
                    z_copy(sgn, t, piece, True).start()

    def z_event(d, piece):
        for sgn in (1, -1):
            o = t - sgn * d

            @pl.when(inside(o))
            def _():
                z_copy(-sgn, o, piece).wait_recv()

                @pl.when(inside(t + sgn))
                def _():
                    z_copy(sgn, o, piece).start()

    def z_drain():
        for piece in range(3):
            for sgn in (1, -1):
                for d in range(n_t - 1):
                    o = t - sgn * d

                    @pl.when(inside(o) & inside(t + sgn))
                    def _():
                        z_copy(sgn, o, piece, d == 0).wait_send()

    def kv_copies(h, m, bit):
        slot = jnp.bitwise_xor(me, m)
        got = m ^ (1 << bit)
        out = []
        for i, (stale, every) in enumerate(((sk_ref, kall), (sv_ref, vall))):
            dst = every.at[slot, pl.ds(h * half, half)]
            src = stale.at[pl.ds(h * half, half)] if m == 0 else dst
            out.append(pltpu.make_async_remote_copy(
                src_ref=src, dst_ref=dst, send_sem=kv_send.at[h, got, i], recv_sem=kv_recv.at[h, got, i],
                device_id=(jnp.bitwise_xor(me, 1 << bit), t), device_id_type=MESH,
            ))
        return out

    def kv_wait(h, m):
        slot = jnp.bitwise_xor(me, m)
        for i, every in enumerate((kall, vall)):
            dst = every.at[slot, pl.ds(h * half, half)]
            pltpu.make_async_remote_copy(
                src_ref=dst, dst_ref=dst, send_sem=kv_send.at[h, m, i], recv_sem=kv_recv.at[h, m, i],
                device_id=(jnp.bitwise_xor(me, 1), t), device_id_type=MESH,
            ).wait_recv()

    def w_copy(k, h, m, bit):
        o = owner(k)
        got = m ^ (1 << bit)
        view = wall_ref.at[o, jnp.bitwise_xor(me, m), :, pl.ds(h * wcols, wcols)]
        return pltpu.make_async_remote_copy(
            src_ref=view, dst_ref=view, send_sem=w_send.at[k, h, got], recv_sem=w_recv.at[k, h, got],
            device_id=(jnp.bitwise_xor(me, 1 << bit), t), device_id_type=MESH,
        )

    def w_wait(k, h, m):
        o = owner(k)
        view = wall_ref.at[o, jnp.bitwise_xor(me, m), :, pl.ds(h * wcols, wcols)]
        pltpu.make_async_remote_copy(
            src_ref=view, dst_ref=view, send_sem=w_send.at[k, h, m], recv_sem=w_recv.at[k, h, m],
            device_id=(jnp.bitwise_xor(me, 1), t), device_id_type=MESH,
        ).wait_recv()

    def fan_out(r):
        out = []
        for pos in range(r.bit_length(), bits - 1):
            out += [(h, orders[h][pos]) for h in (0, 1)]
        return out + [(0, 0), (1, 0)]

    def kv_event(r):
        if r:
            for h in (0, 1):
                kv_wait(h, unrank(h, r))
        for h, bit in fan_out(r):
            for copy in kv_copies(h, unrank(h, r), bit):
                copy.start()

    def w_event(k, r):
        if r:
            for h in (0, 1):
                w_wait(k, h, unrank(h, r))
        for h, bit in fan_out(r):
            w_copy(k, h, unrank(h, r), bit).start()

    def core_wait(r):
        for h in (0, 1):
            kv_wait(h, unrank(h, r) ^ 1)

    def text_copies(i, act):
        peer = jnp.bitwise_xor(me, i)
        for j, ref in enumerate((tk, tv)):
            src = ref.at[pl.ds(pl.multiple_of(me * trows, trows), trows)]
            dst = ref.at[pl.ds(pl.multiple_of(me * trows, trows), trows)]
            act(pltpu.make_async_remote_copy(
                src_ref=src, dst_ref=dst, send_sem=tx_send.at[i, j], recv_sem=tx_recv.at[i, j],
                device_id=(peer, t), device_id_type=MESH,
            ))

    def text_wait(i):
        peer = jnp.bitwise_xor(me, i)
        for j, ref in enumerate((tk, tv)):
            dst = ref.at[pl.ds(pl.multiple_of(peer * trows, trows), trows)]
            pltpu.make_async_remote_copy(
                src_ref=dst, dst_ref=dst, send_sem=tx_send.at[i, j], recv_sem=tx_recv.at[i, j],
                device_id=(peer, t), device_id_type=MESH,
            ).wait_recv()

    def a_copy(o, u):
        span = pl.ds(u * hrows, hrows)
        return pltpu.make_async_remote_copy(
            src_ref=asend.at[o, span], dst_ref=att_ref.at[t, span], send_sem=a_send.at[o, u], recv_sem=a_recv.at[t, u],
            device_id=(me, o), device_id_type=MESH,
        )

    def a_wait(o, u):
        span = pl.ds(u * hrows, hrows)
        pltpu.make_async_remote_copy(
            src_ref=asend.at[o, span], dst_ref=att_ref.at[o, span], send_sem=a_send.at[o, u], recv_sem=a_recv.at[o, u],
            device_id=(me, o), device_id_type=MESH,
        ).wait_recv()

    def qkv(x_view, rs, n):
        def part(j, carry):
            prod = jnp.dot(x_view[...], w[j], preferred_element_type=jnp.float32)
            gain = jnp.where(j == 0, qg_ref[...], kg_ref[...])
            for h in range(heads):
                c = slice(h * hd, (h + 1) * hd)
                piece = prod[:, c]
                value = jnp.where(j == 2, piece, rms_gain(piece, gain)).astype(jnp.bfloat16)

                @pl.when(j == 0)
                def _():
                    q_ref[pl.ds(rs, n), c] = value

                @pl.when(j == 1)
                def _():
                    kall[me, pl.ds(rs, n), c] = value

                @pl.when(j == 2)
                def _():
                    vall[me, pl.ds(rs, n), c] = value
            return carry

        lax.fori_loop(0, 3, part, 0)

    def block_start(k):
        return pl.multiple_of(owner(k) * rows, rows)

    def whole_slot(m):
        slot = jnp.bitwise_xor(me, m)
        return (kall.at[slot], vall.at[slot])

    def fresh_span(k):
        first = t
        for j in range(1, k):
            first = jnp.minimum(first, owner(j))
        span = pl.ds(pl.multiple_of(first * rows, rows), k * rows)
        return (kall.at[me, span], vall.at[me, span])

    def fresh_block(k):
        span = pl.ds(block_start(k), rows)
        return (kall.at[me, span], vall.at[me, span])

    def attend(rs, n, chunks, first=False, final=None, unroll=False):
        def compute(c):
            q = q_ref[pl.ds(rs, n), c]

            def score(chunk):
                return lax.dot_general(
                    q, chunk[0][:, c], (((1,), (1,)), ((), ())), preferred_element_type=jnp.float32
                )

            if first:
                peak = jnp.full((n, hd), -1e30, jnp.float32)
                denom = jnp.zeros((n, hd), jnp.float32)
                numer = jnp.zeros((n, hd), jnp.float32)
            else:
                peak = m_ref[pl.ds(rs, n), c]
                denom = l_ref[pl.ds(rs, n), c]
                numer = acc_ref[pl.ds(rs, n), c]
            ahead = score(chunks[0])
            for idx, chunk in enumerate(chunks):
                scores = ahead
                if idx + 1 < len(chunks):
                    ahead = score(chunks[idx + 1])
                high = jnp.broadcast_to(jnp.max(scores, axis=-1, keepdims=True), (n, hd))
                new_peak = jnp.maximum(peak, high)
                rescale = jnp.exp2((peak - new_peak) * scale)
                denom = denom * rescale
                step = scores.shape[1]
                parts = []
                for lane in range(0, step, hd):
                    wide = min(hd, step - lane)
                    part = jnp.exp2((scores[:, lane : lane + wide] - new_peak[:, :wide]) * scale)
                    denom = denom + (part if wide == hd else jnp.pad(part, ((0, 0), (0, hd - wide))))
                    parts.append(part.astype(jnp.bfloat16))
                numer = numer * rescale + jnp.dot(
                    jnp.concatenate(parts, axis=1), chunk[1][:, c], preferred_element_type=jnp.float32
                )
                peak = new_peak
            if final is not None:
                return ((numer / jnp.sum(denom, axis=-1, keepdims=True)).astype(jnp.bfloat16),)
            return (peak, denom, numer)

        def store(c, values):
            if final is not None:
                o, top = final
                asend[o, pl.ds(top, n), c] = values[0]
            else:
                for ref, value in zip((m_ref, l_ref, acc_ref), values):
                    ref[pl.ds(rs, n), c] = value

        if unroll:
            spans = [slice(h * hd, (h + 1) * hd) for h in range(heads)]
            results = [compute(c) for c in spans]
            for c, values in zip(spans, results):
                store(c, values)
            return

        def head(h, carry):
            c = pl.ds(pl.multiple_of(h * hd, hd), hd)
            store(c, compute(c))
            return carry

        lax.fori_loop(0, heads, head, 0)

    load_w = pltpu.make_async_copy(w_hbm, w, load_sem.at[0])
    load_t = pltpu.make_async_copy(wt_hbm, wt, load_sem.at[1])
    load_t.start()
    load_w.start()
    kv_event(0)
    strip = min(hrows, 32)

    def mod_strip(i, carry):
        span = pl.ds(pl.multiple_of(i * strip, strip), strip)
        xall[t, span] = layer_mod(x_ref[span], ishift_ref[...], iscale_ref[...])
        return carry

    lax.fori_loop(0, rows // strip, mod_strip, 0)
    z_start((0, 1, 2))

    text_mod = layer_mod(text_ref[...], tshift_ref[...], tscale_ref[...])
    ts = pl.multiple_of(me * trows, trows)
    load_t.wait()
    for j, ref in enumerate((tk, tv)):
        prod = jnp.dot(text_mod, wt[:, j, :], preferred_element_type=jnp.float32)
        for h in range(heads):
            c = slice(h * hd, (h + 1) * hd)
            piece = prod[:, c]
            if j == 0:
                piece = rms_gain(piece, tg_ref[...])
            ref[pl.ds(ts, trows), c] = piece.astype(jnp.bfloat16)
    load_w.wait()
    qkv(xall.at[t], block_start(0), rows)

    early = n_t // 2
    last = n_t - 1
    full = n_p - 2
    near = [whole_slot(1)]
    main = [whole_slot(m) for m in range(2, full)]
    rest = [whole_slot(m) for m in range(full, n_p)]
    text = [(tk, tv)]

    z_event(1, 0)
    kv_event(1)

    def text_start(i, carry):
        text_copies(i, lambda copy: copy.start())
        return carry

    lax.fori_loop(1, n_p, text_start, 0)
    core_wait(0)
    attend(block_start(0), rows, near + [fresh_block(0)], first=True)
    z_event(1, 1)
    for d in range(1, early):
        if d > 1:
            z_event(d, 0)
            z_event(d, 1)
        qkv(xall.at[owner(d)], block_start(d), rows)
        attend(block_start(d), rows, near + [fresh_block(0)], first=True)
    for d in range(1, early):
        z_event(d, 2)
        w_event(d, 0)
    for r in range(2, last_rank - 1):
        kv_event(r)
    for r in range(1, last_rank - 1):
        core_wait(r)

    def grown(k, final, extra, unroll=True):
        def older(j, carry):
            o = owner(j)
            attend(block_start(j), rows, [fresh_block(k)] + extra, final=(o, 0) if final else None, unroll=unroll)
            if final:
                @pl.when(o != t)
                def _():
                    for u in (0, 1):
                        a_copy(o, u).start()
            return carry

        lax.fori_loop(0, k, older, 0)

    def early_main(k, carry):
        attend(block_start(k), rows, main)
        return carry

    lax.fori_loop(0, early, early_main, 0)
    z_event(early, 0)
    kv_event(last_rank - 1)
    core_wait(last_rank - 1)

    def early_rest(k, carry):
        attend(block_start(k), rows, rest)
        return carry

    lax.fori_loop(0, early, early_rest, 0)
    for d in range(1, early):
        w_event(d, 1)
    z_event(early, 1)

    def text_done(i, carry):
        text_wait(i)
        return carry

    lax.fori_loop(1, n_p, text_done, 0)

    def early_fresh(j, carry):
        others = [fresh_block(d) for d in range(1, early)]
        attend(block_start(j), rows, others + text, unroll=True)
        return carry

    for k in range(early, last):
        if k > early:
            z_event(k, 0)
            z_event(k, 1)
        qkv(xall.at[owner(k)], block_start(k), rows)
        z_event(k, 2)
        w_event(k, 0)
        if k == early:
            for d in range(1, early):
                w_event(d, 2)
            lax.fori_loop(0, early, early_fresh, 0)
            for r in range(3, last_rank):
                for d in range(1, early):
                    w_event(d, r)
        grown(k, False, [])
        attend(block_start(k), rows, near + main + rest + text + [fresh_span(k + 1)], first=True)
        w_event(k, 1)

    far = owner(last)
    z_event(last, 0)
    rs_a = block_start(last)
    rs_b = pl.multiple_of(rs_a + hrows, hrows)
    qkv(xall.at[far, pl.ds(0, hrows)], rs_a, hrows)
    attend(rs_a, hrows, near + main + rest + text, first=True)
    for r in range(2, last_rank):
        for k in range(early, last):
            w_event(k, r)
    z_event(last, 1)
    qkv(xall.at[far, pl.ds(hrows, hrows)], rs_b, hrows)
    grown(last, True, [])
    attend(rs_a, hrows, [whole_slot(0)], final=(far, 0), unroll=True)
    a_copy(far, 0).start()
    attend(rs_b, hrows, near + main, first=True)
    z_event(last, 2)
    w_event(last, 0)
    attend(rs_b, hrows, rest + text + [whole_slot(0)], final=(far, hrows))
    a_copy(far, 1).start()
    for r in range(1, last_rank):
        w_event(last, r)

    own_att = pltpu.make_async_copy(asend.at[t], att_ref.at[t], out_sem.at[0])
    put_k = pltpu.make_async_copy(kall.at[me], nk_ref, out_sem.at[1])
    put_v = pltpu.make_async_copy(vall.at[me], nv_ref, out_sem.at[2])
    for copy in (own_att, put_k, put_v):
        copy.start()

    for k in range(1, n_t):
        for r in range(last_rank):
            for h in (0, 1):
                w_wait(k, h, unrank(h, r) ^ 1)
    z_drain()
    for r in range(last_rank):
        for h, bit in fan_out(r):
            for copy in kv_copies(h, unrank(h, r), bit):
                copy.wait_send()
    for k in range(1, n_t):
        for r in range(last_rank):
            for h, bit in fan_out(r):
                w_copy(k, h, unrank(h, r), bit).wait_send()

    def text_sent(i, carry):
        text_copies(i, lambda copy: copy.wait_send())
        return carry

    lax.fori_loop(1, n_p, text_sent, 0)
    for copy in (own_att, put_k, put_v):
        copy.wait()

    def a_done(i, carry):
        o = lax.rem(t + i, n_t)
        for u in (0, 1):
            a_copy(o, u).wait_send()
            a_wait(o, u)
        return carry

    lax.fori_loop(1, n_t, a_done, 0)


def fused(n_p, n_t, x, ishift, iscale, text, tshift, tscale, w, wt, q_gain, k_gain, t_gain, out_weight, stale_k, stale_v):
    rows, width = x.shape
    keys, cols = stale_k.shape
    hd = q_gain.shape[0]
    trows = text.shape[0]
    share = out_weight.shape[0] // n_p
    scale = math.log2(math.e) / float(hd) ** 0.5
    bf16, f32 = jnp.bfloat16, jnp.float32
    dma = pltpu.SemaphoreType.DMA
    return pl.pallas_call(
        functools.partial(fused_kernel, n_p, n_t, scale),
        out_shape=(
            jax.ShapeDtypeStruct((keys, cols), bf16),
            jax.ShapeDtypeStruct((keys, cols), bf16),
            jax.ShapeDtypeStruct((n_t, rows, cols), bf16),
            jax.ShapeDtypeStruct((n_t, n_p, share, width), bf16),
        ),
        in_specs=[VMEM, VMEM, VMEM, VMEM, VMEM, VMEM, ANY, ANY, VMEM, VMEM, VMEM, ANY, ANY, ANY],
        out_specs=(ANY,) * 4,
        scratch_shapes=[
            pltpu.VMEM((n_t, rows, width), bf16),
            pltpu.VMEM(w.shape, bf16),
            pltpu.VMEM(wt.shape, bf16),
            pltpu.VMEM((n_p, keys, cols), bf16),
            pltpu.VMEM((n_p, keys, cols), bf16),
            pltpu.VMEM((n_p * trows, cols), bf16),
            pltpu.VMEM((n_p * trows, cols), bf16),
            pltpu.VMEM((keys, cols), bf16),
            pltpu.VMEM((keys, cols), f32),
            pltpu.VMEM((keys, cols), f32),
            pltpu.VMEM((keys, cols), f32),
            pltpu.VMEM((n_t, rows, cols), bf16),
            dma((2,)),
            dma((2, n_p, 2)),
            dma((2, n_p, 2)),
            dma((2, n_t, 3)),
            dma((n_t, 3)),
            dma((n_p, 2)),
            dma((n_p, 2)),
            dma((n_t, 2, n_p)),
            dma((n_t, 2, n_p)),
            dma((n_t, 2)),
            dma((n_t, 2)),
            dma((3,)),
        ],
        compiler_params=pltpu.CompilerParams(
            collective_id=0, has_side_effects=True, vmem_limit_bytes=63 * 1024 * 1024
        ),
        name="fused",
    )(x, ishift[None, :], iscale[None, :], text, tshift[None, :], tscale[None, :], w, wt, q_gain[None, :], k_gain[None, :], t_gain[None, :],
      out_weight, stale_k, stale_v)


def finish_kernel(n_t, x_ref, nk_ref, nv_ref, ow_ref, t_ref, g_ref, *refs):
    t = lax.axis_index("tensor")
    walls, (o_ref, ko_ref, vo_ref) = refs[: n_t - 1], refs[n_t - 1 :]
    total = jnp.dot(x_ref[t], ow_ref[...], preferred_element_type=jnp.float32)
    for j in range(1, n_t):
        total = total + jnp.dot(x_ref[lax.rem(t + j, n_t)], walls[j - 1][0], preferred_element_type=jnp.float32)
    o_ref[...] = (t_ref[...].astype(jnp.float32) + g_ref[...] * total).astype(jnp.bfloat16)
    ko_ref[...] = nk_ref[...]
    vo_ref[...] = nv_ref[...]


def finish(att, wall, out_weight, tokens, gate, new_k, new_v):
    n_t, rows, depth = att.shape
    width = tokens.shape[1]
    keys, cols = new_k.shape
    steps = 6 if width % 6 == 0 and (width // 6) % 128 == 0 and keys % 96 == 0 else 4
    tile = width // steps
    part = pl.BlockSpec((keys // steps, cols), lambda j: (j, 0))

    def other(i):
        def index(j):
            return (lax.rem(lax.axis_index("tensor") + i, n_t), 0, j)

        return pl.BlockSpec((1, depth, tile), index)

    return pl.pallas_call(
        functools.partial(finish_kernel, n_t),
        grid=(steps,),
        out_shape=(
            jax.ShapeDtypeStruct(tokens.shape, jnp.bfloat16),
            jax.ShapeDtypeStruct(new_k.shape, jnp.bfloat16),
            jax.ShapeDtypeStruct(new_v.shape, jnp.bfloat16),
        ),
        in_specs=[
            pl.BlockSpec((n_t, rows, depth), lambda j: (0, 0, 0)),
            part,
            part,
            pl.BlockSpec((depth, tile), lambda j: (0, j)),
            pl.BlockSpec((rows, tile), lambda j: (0, j)),
            pl.BlockSpec((1, tile), lambda j: (0, j)),
        ]
        + [other(i) for i in range(1, n_t)],
        out_specs=(pl.BlockSpec((rows, tile), lambda j: (0, j)), part, part),
        name="finish",
    )(att, new_k, new_v, out_weight, tokens, gate[None, :], *[wall] * (n_t - 1))


def per_device(
    n_patch,
    n_tensor,
    tokens,
    text_tokens,
    img_shift,
    img_scale,
    img_gate,
    txt_shift,
    txt_scale,
    qkv_weight,
    txt_kv_weight,
    q_gain,
    k_gain,
    txt_k_gain,
    out_weight,
    stale_keys,
    stale_values,
):
    new_keys, new_values, att, wall = fused(
        n_patch, n_tensor, tokens, img_shift, img_scale, text_tokens, txt_shift, txt_scale,
        jnp.transpose(qkv_weight, (1, 0, 2)), txt_kv_weight,
        q_gain, k_gain, txt_k_gain, out_weight, stale_keys, stale_values,
    )
    wall = wall.reshape(n_tensor, -1, wall.shape[-1])
    return finish(att, wall, out_weight, tokens, img_gate, new_keys, new_values)


def solution(mesh):
    placed = (
        P(("patch", "tensor"), None),
        P("patch", None),
        P(),
        P(),
        P(),
        P(),
        P(),
        P(None, None, "tensor"),
        P(None, None, "tensor"),
        P(),
        P(),
        P(),
        P("tensor", None),
        P("patch", "tensor"),
        P("patch", "tensor"),
    )
    return jax.shard_map(
        functools.partial(per_device, mesh.shape["patch"], mesh.shape["tensor"]),
        mesh=mesh,
        in_specs=placed,
        out_specs=(P(("patch", "tensor"), None), P("patch", "tensor"), P("patch", "tensor")),
        check_vma=False,
    )
```

```python
import functools
import math

import jax
import jax.numpy as jnp
from jax import lax
from jax.experimental import pallas as pl
from jax.experimental.pallas import tpu as pltpu
from jax.sharding import PartitionSpec as P

MESH = pl.DeviceIdType.MESH
ANY = pl.BlockSpec(memory_space=pl.ANY)
VMEM = pl.BlockSpec(memory_space=pltpu.VMEM)


def layer_mod(values, shift_vec, scale_vec):
    wide = values.astype(jnp.float32)
    centre = jnp.mean(wide, axis=-1, keepdims=True)
    off = wide - centre
    spread = jnp.mean(off * off, axis=-1, keepdims=True)
    return ((1.0 + scale_vec) * (off * lax.rsqrt(spread + 1e-06)) + shift_vec).astype(jnp.bfloat16)


def rms_gain(piece, gain):
    square = jnp.mean(piece * piece, axis=-1, keepdims=True)
    return piece * lax.rsqrt(square + 1e-06) * gain


def fused_kernel(
    n_p, n_t, scale,
    x_ref, ishift_ref, iscale_ref, text_ref, tshift_ref, tscale_ref, w_hbm, wt_hbm, qg_ref, kg_ref, tg_ref, ow_ref, sk_ref, sv_ref,
    nk_ref, nv_ref, att_ref, wall_ref,
    xall, w, wt, kall, vall, tk, tv, q_ref, m_ref, l_ref, acc_ref, asend,
    load_sem, kv_send, kv_recv, z_send, z_recv, tx_send, tx_recv, w_send, w_recv, a_send, a_recv, out_sem,
):
    me = lax.axis_index("patch")
    t = lax.axis_index("tensor")
    rows, width = x_ref.shape
    keys, cols = sk_ref.shape
    hd = qg_ref.shape[1]
    heads = cols // hd
    half = keys // 2
    hrows = rows // 2
    trows = text_ref.shape[0]
    share = ow_ref.shape[0] // n_p
    wcols = width // 2
    bits = n_p.bit_length() - 1
    orders = (list(range(1, bits)), list(range(1, bits))[::-1])
    last_rank = 1 << (bits - 1)

    def unrank(h, r):
        return sum(1 << b for pos, b in enumerate(orders[h]) if r >> pos & 1)

    def owner(k):
        lo, hi = t, n_t - 1 - t
        near = jnp.minimum(lo, hi)
        step = lax.div(k + 1, 2)
        both = jnp.where(lax.rem(k, 2) == 1, t - step, t + step)
        one = jnp.where(lo <= hi, t + (k - near), t - (k - near))
        return jnp.where(k <= 2 * near, both, one)

    bar = pltpu.get_barrier_semaphore()

    def greet_patch(i, c):
        pl.semaphore_signal(bar, inc=1, device_id=(jnp.bitwise_xor(me, i), t), device_id_type=MESH)
        return c

    def greet_tensor(i, c):
        pl.semaphore_signal(bar, inc=1, device_id=(me, lax.rem(t + i, n_t)), device_id_type=MESH)
        return c

    lax.fori_loop(1, n_p, greet_patch, 0)
    lax.fori_loop(1, n_t, greet_tensor, 0)
    pl.semaphore_wait(bar, n_p + n_t - 2)

    def z_views(o, piece):
        if piece < 2:
            ref = xall.at[o, pl.ds(piece * hrows, hrows)]
        else:
            ref = wall_ref.at[o, me]
        return ref

    def z_copy(sgn, o, piece, first=False):
        dst = z_views(o, piece)
        src = dst
        if first:
            if piece == 2:
                src = ow_ref.at[pl.ds(pl.multiple_of(me * share, share), share)]
        d = (sgn + 1) // 2
        return pltpu.make_async_remote_copy(
            src_ref=src, dst_ref=dst, send_sem=z_send.at[d, o, piece], recv_sem=z_recv.at[o, piece],
            device_id=(me, t + sgn), device_id_type=MESH,
        )

    def inside(i):
        return (i >= 0) & (i < n_t)

    def z_start(pieces):
        for piece in pieces:
            for sgn in (-1, 1):
                @pl.when(inside(t + sgn))
                def _():
                    z_copy(sgn, t, piece, True).start()

    def z_event(d, piece):
        for sgn in (1, -1):
            o = t - sgn * d

            @pl.when(inside(o))
            def _():
                z_copy(-sgn, o, piece).wait_recv()

                @pl.when(inside(t + sgn))
                def _():
                    z_copy(sgn, o, piece).start()

    def z_drain():
        for piece in range(3):
            for sgn in (1, -1):
                for d in range(n_t - 1):
                    o = t - sgn * d

                    @pl.when(inside(o) & inside(t + sgn))
                    def _():
                        z_copy(sgn, o, piece, d == 0).wait_send()

    def kv_copies(h, m, bit):
        slot = jnp.bitwise_xor(me, m)
        got = m ^ (1 << bit)
        out = []
        for i, (stale, every) in enumerate(((sk_ref, kall), (sv_ref, vall))):
            dst = every.at[slot, pl.ds(h * half, half)]
            src = stale.at[pl.ds(h * half, half)] if m == 0 else dst
            out.append(pltpu.make_async_remote_copy(
                src_ref=src, dst_ref=dst, send_sem=kv_send.at[h, got, i], recv_sem=kv_recv.at[h, got, i],
                device_id=(jnp.bitwise_xor(me, 1 << bit), t), device_id_type=MESH,
            ))
        return out

    def kv_wait(h, m):
        slot = jnp.bitwise_xor(me, m)
        for i, every in enumerate((kall, vall)):
            dst = every.at[slot, pl.ds(h * half, half)]
            pltpu.make_async_remote_copy(
                src_ref=dst, dst_ref=dst, send_sem=kv_send.at[h, m, i], recv_sem=kv_recv.at[h, m, i],
                device_id=(jnp.bitwise_xor(me, 1), t), device_id_type=MESH,
            ).wait_recv()

    def w_copy(k, h, m, bit):
        o = owner(k)
        got = m ^ (1 << bit)
        view = wall_ref.at[o, jnp.bitwise_xor(me, m), :, pl.ds(h * wcols, wcols)]
        return pltpu.make_async_remote_copy(
            src_ref=view, dst_ref=view, send_sem=w_send.at[k, h, got], recv_sem=w_recv.at[k, h, got],
            device_id=(jnp.bitwise_xor(me, 1 << bit), t), device_id_type=MESH,
        )

    def w_wait(k, h, m):
        o = owner(k)
        view = wall_ref.at[o, jnp.bitwise_xor(me, m), :, pl.ds(h * wcols, wcols)]
        pltpu.make_async_remote_copy(
            src_ref=view, dst_ref=view, send_sem=w_send.at[k, h, m], recv_sem=w_recv.at[k, h, m],
            device_id=(jnp.bitwise_xor(me, 1), t), device_id_type=MESH,
        ).wait_recv()

    def fan_out(r):
        out = []
        for pos in range(r.bit_length(), bits - 1):
            out += [(h, orders[h][pos]) for h in (0, 1)]
        return out + [(0, 0), (1, 0)]

    def kv_event(r):
        if r:
            for h in (0, 1):
                kv_wait(h, unrank(h, r))
        for h, bit in fan_out(r):
            for copy in kv_copies(h, unrank(h, r), bit):
                copy.start()

    def w_event(k, r):
        if r:
            for h in (0, 1):
                w_wait(k, h, unrank(h, r))
        for h, bit in fan_out(r):
            w_copy(k, h, unrank(h, r), bit).start()

    def core_wait(r):
        for h in (0, 1):
            kv_wait(h, unrank(h, r) ^ 1)

    def text_copies(i, act):
        peer = jnp.bitwise_xor(me, i)
        for j, ref in enumerate((tk, tv)):
            src = ref.at[pl.ds(pl.multiple_of(me * trows, trows), trows)]
            dst = ref.at[pl.ds(pl.multiple_of(me * trows, trows), trows)]
            act(pltpu.make_async_remote_copy(
                src_ref=src, dst_ref=dst, send_sem=tx_send.at[i, j], recv_sem=tx_recv.at[i, j],
                device_id=(peer, t), device_id_type=MESH,
            ))

    def text_wait(i):
        peer = jnp.bitwise_xor(me, i)
        for j, ref in enumerate((tk, tv)):
            dst = ref.at[pl.ds(pl.multiple_of(peer * trows, trows), trows)]
            pltpu.make_async_remote_copy(
                src_ref=dst, dst_ref=dst, send_sem=tx_send.at[i, j], recv_sem=tx_recv.at[i, j],
                device_id=(peer, t), device_id_type=MESH,
            ).wait_recv()

    def a_copy(o, u):
        span = pl.ds(u * hrows, hrows)
        return pltpu.make_async_remote_copy(
            src_ref=asend.at[o, span], dst_ref=att_ref.at[t, span], send_sem=a_send.at[o, u], recv_sem=a_recv.at[t, u],
            device_id=(me, o), device_id_type=MESH,
        )

    def a_wait(o, u):
        span = pl.ds(u * hrows, hrows)
        pltpu.make_async_remote_copy(
            src_ref=asend.at[o, span], dst_ref=att_ref.at[o, span], send_sem=a_send.at[o, u], recv_sem=a_recv.at[o, u],
            device_id=(me, o), device_id_type=MESH,
        ).wait_recv()

    def qkv(x_view, rs, n):
        def part(j, carry):
            prod = jnp.dot(x_view[...], w[j], preferred_element_type=jnp.float32)
            gain = jnp.where(j == 0, qg_ref[...], kg_ref[...])
            for h in range(heads):
                c = slice(h * hd, (h + 1) * hd)
                piece = prod[:, c]
                value = jnp.where(j == 2, piece, rms_gain(piece, gain)).astype(jnp.bfloat16)

                @pl.when(j == 0)
                def _():
                    q_ref[pl.ds(rs, n), c] = value

                @pl.when(j == 1)
                def _():
                    kall[me, pl.ds(rs, n), c] = value

                @pl.when(j == 2)
                def _():
                    vall[me, pl.ds(rs, n), c] = value
            return carry

        lax.fori_loop(0, 3, part, 0)

    def block_start(k):
        return pl.multiple_of(owner(k) * rows, rows)

    def whole_slot(m):
        slot = jnp.bitwise_xor(me, m)
        return (kall.at[slot], vall.at[slot])

    def fresh_span(k):
        first = t
        for j in range(1, k):
            first = jnp.minimum(first, owner(j))
        span = pl.ds(pl.multiple_of(first * rows, rows), k * rows)
        return (kall.at[me, span], vall.at[me, span])

    def fresh_block(k):
        span = pl.ds(block_start(k), rows)
        return (kall.at[me, span], vall.at[me, span])

    def attend(rs, n, chunks, first=False, final=None, unroll=False):
        def compute(c):
            q = q_ref[pl.ds(rs, n), c]

            def score(chunk):
                return lax.dot_general(
                    q, chunk[0][:, c], (((1,), (1,)), ((), ())), preferred_element_type=jnp.float32
                )

            if first:
                peak = jnp.full((n, hd), -1e30, jnp.float32)
                denom = jnp.zeros((n, hd), jnp.float32)
                numer = jnp.zeros((n, hd), jnp.float32)
            else:
                peak = m_ref[pl.ds(rs, n), c]
                denom = l_ref[pl.ds(rs, n), c]
                numer = acc_ref[pl.ds(rs, n), c]
            ahead = score(chunks[0])
            for idx, chunk in enumerate(chunks):
                scores = ahead
                if idx + 1 < len(chunks):
                    ahead = score(chunks[idx + 1])
                high = jnp.broadcast_to(jnp.max(scores, axis=-1, keepdims=True), (n, hd))
                new_peak = jnp.maximum(peak, high)
                rescale = jnp.exp2((peak - new_peak) * scale)
                denom = denom * rescale
                step = scores.shape[1]
                parts = []
                for lane in range(0, step, hd):
                    wide = min(hd, step - lane)
                    part = jnp.exp2((scores[:, lane : lane + wide] - new_peak[:, :wide]) * scale)
                    denom = denom + (part if wide == hd else jnp.pad(part, ((0, 0), (0, hd - wide))))
                    parts.append(part.astype(jnp.bfloat16))
                numer = numer * rescale + jnp.dot(
                    jnp.concatenate(parts, axis=1), chunk[1][:, c], preferred_element_type=jnp.float32
                )
                peak = new_peak
            if final is not None:
                return ((numer / jnp.sum(denom, axis=-1, keepdims=True)).astype(jnp.bfloat16),)
            return (peak, denom, numer)

        def store(c, values):
            if final is not None:
                o, top = final
                asend[o, pl.ds(top, n), c] = values[0]
            else:
                for ref, value in zip((m_ref, l_ref, acc_ref), values):
                    ref[pl.ds(rs, n), c] = value

        if unroll:
            spans = [slice(h * hd, (h + 1) * hd) for h in range(heads)]
            results = [compute(c) for c in spans]
            for c, values in zip(spans, results):
                store(c, values)
            return

        def head(h, carry):
            c = pl.ds(pl.multiple_of(h * hd, hd), hd)
            store(c, compute(c))
            return carry

        lax.fori_loop(0, heads, head, 0)

    load_w = pltpu.make_async_copy(w_hbm, w, load_sem.at[0])
    load_t = pltpu.make_async_copy(wt_hbm, wt, load_sem.at[1])
    load_t.start()
    load_w.start()
    kv_event(0)
    strip = min(hrows, 32)

    def mod_strip(i, carry):
        span = pl.ds(pl.multiple_of(i * strip, strip), strip)
        xall[t, span] = layer_mod(x_ref[span], ishift_ref[...], iscale_ref[...])
        return carry

    lax.fori_loop(0, rows // strip, mod_strip, 0)
    z_start((0, 1, 2))

    text_mod = layer_mod(text_ref[...], tshift_ref[...], tscale_ref[...])
    ts = pl.multiple_of(me * trows, trows)
    load_t.wait()
    for j, ref in enumerate((tk, tv)):
        prod = jnp.dot(text_mod, wt[:, j, :], preferred_element_type=jnp.float32)
        for h in range(heads):
            c = slice(h * hd, (h + 1) * hd)
            piece = prod[:, c]
            if j == 0:
                piece = rms_gain(piece, tg_ref[...])
            ref[pl.ds(ts, trows), c] = piece.astype(jnp.bfloat16)
    load_w.wait()
    qkv(xall.at[t], block_start(0), rows)

    early = n_t // 2
    last = n_t - 1
    full = n_p - 2
    near = [whole_slot(1)]
    main = [whole_slot(m) for m in range(2, full)]
    rest = [whole_slot(m) for m in range(full, n_p)]
    text = [(tk, tv)]

    z_event(1, 0)
    kv_event(1)

    def text_start(i, carry):
        text_copies(i, lambda copy: copy.start())
        return carry

    lax.fori_loop(1, n_p, text_start, 0)
    core_wait(0)
    attend(block_start(0), rows, near + [fresh_block(0)], first=True)
    z_event(1, 1)
    for d in range(1, early):
        if d > 1:
            z_event(d, 0)
            z_event(d, 1)
        qkv(xall.at[owner(d)], block_start(d), rows)
        attend(block_start(d), rows, near + [fresh_block(0)], first=True)
    for d in range(1, early):
        z_event(d, 2)
        w_event(d, 0)
    for r in range(2, last_rank - 1):
        kv_event(r)
    for r in range(1, last_rank - 1):
        core_wait(r)

    def grown(k, final, extra, unroll=True):
        def older(j, carry):
            o = owner(j)
            attend(block_start(j), rows, [fresh_block(k)] + extra, final=(o, 0) if final else None, unroll=unroll)
            if final:
                @pl.when(o != t)
                def _():
                    for u in (0, 1):
                        a_copy(o, u).start()
            return carry

        lax.fori_loop(0, k, older, 0)

    def early_main(k, carry):
        attend(block_start(k), rows, main)
        return carry

    lax.fori_loop(0, early, early_main, 0)
    z_event(early, 0)
    kv_event(last_rank - 1)
    core_wait(last_rank - 1)

    def early_rest(k, carry):
        attend(block_start(k), rows, rest)
        return carry

    lax.fori_loop(0, early, early_rest, 0)
    for d in range(1, early):
        w_event(d, 1)
    z_event(early, 1)

    def text_done(i, carry):
        text_wait(i)
        return carry

    lax.fori_loop(1, n_p, text_done, 0)

    def early_fresh(j, carry):
        others = [fresh_block(d) for d in range(1, early)]
        attend(block_start(j), rows, others + text, unroll=True)
        return carry

    for k in range(early, last):
        if k > early:
            z_event(k, 0)
            z_event(k, 1)
        qkv(xall.at[owner(k)], block_start(k), rows)
        z_event(k, 2)
        w_event(k, 0)
        if k == early:
            for d in range(1, early):
                w_event(d, 2)
            lax.fori_loop(0, early, early_fresh, 0)
            for r in range(3, last_rank):
                for d in range(1, early):
                    w_event(d, r)
        grown(k, False, [])
        attend(block_start(k), rows, near + main + rest + text + [fresh_span(k + 1)], first=True)
        w_event(k, 1)

    far = owner(last)
    z_event(last, 0)
    rs_a = block_start(last)
    rs_b = pl.multiple_of(rs_a + hrows, hrows)

    def tail(u, carry):
        @pl.when(u == 1)
        def _():
            z_event(last, 1)

        top = pl.multiple_of(u * hrows, hrows)
        rs = pl.multiple_of(rs_a + top, hrows)
        qkv(xall.at[far, pl.ds(top, hrows)], rs, hrows)

        @pl.when(u == 1)
        def _():
            grown(last, True, [])
            attend(rs_a, hrows, [whole_slot(0)], final=(far, 0), unroll=True)
            a_copy(far, 0).start()
            z_event(last, 2)
            w_event(last, 0)

        attend(rs, hrows, near + main + rest + text, first=True)

        @pl.when(u == 0)
        def _():
            for r in range(2, last_rank):
                for k in range(early, last):
                    w_event(k, r)
        return carry

    lax.fori_loop(0, 2, tail, 0)
    w_event(last, 1)
    attend(rs_b, hrows, [whole_slot(0)], final=(far, hrows), unroll=True)
    a_copy(far, 1).start()
    for r in range(2, last_rank):
        w_event(last, r)

    own_att = pltpu.make_async_copy(asend.at[t], att_ref.at[t], out_sem.at[0])
    put_k = pltpu.make_async_copy(kall.at[me], nk_ref, out_sem.at[1])
    put_v = pltpu.make_async_copy(vall.at[me], nv_ref, out_sem.at[2])
    for copy in (own_att, put_k, put_v):
        copy.start()

    for k in range(1, n_t):
        for r in range(last_rank):
            for h in (0, 1):
                w_wait(k, h, unrank(h, r) ^ 1)
    z_drain()
    for r in range(last_rank):
        for h, bit in fan_out(r):
            for copy in kv_copies(h, unrank(h, r), bit):
                copy.wait_send()
    for k in range(1, n_t):
        for r in range(last_rank):
            for h, bit in fan_out(r):
                w_copy(k, h, unrank(h, r), bit).wait_send()

    def text_sent(i, carry):
        text_copies(i, lambda copy: copy.wait_send())
        return carry

    lax.fori_loop(1, n_p, text_sent, 0)
    for copy in (own_att, put_k, put_v):
        copy.wait()

    def a_done(i, carry):
        o = lax.rem(t + i, n_t)
        for u in (0, 1):
            a_copy(o, u).wait_send()
            a_wait(o, u)
        return carry

    lax.fori_loop(1, n_t, a_done, 0)


def fused(n_p, n_t, x, ishift, iscale, text, tshift, tscale, w, wt, q_gain, k_gain, t_gain, out_weight, stale_k, stale_v):
    rows, width = x.shape
    keys, cols = stale_k.shape
    hd = q_gain.shape[0]
    trows = text.shape[0]
    share = out_weight.shape[0] // n_p
    scale = math.log2(math.e) / float(hd) ** 0.5
    bf16, f32 = jnp.bfloat16, jnp.float32
    dma = pltpu.SemaphoreType.DMA
    return pl.pallas_call(
        functools.partial(fused_kernel, n_p, n_t, scale),
        out_shape=(
            jax.ShapeDtypeStruct((keys, cols), bf16),
            jax.ShapeDtypeStruct((keys, cols), bf16),
            jax.ShapeDtypeStruct((n_t, rows, cols), bf16),
            jax.ShapeDtypeStruct((n_t, n_p, share, width), bf16),
        ),
        in_specs=[VMEM, VMEM, VMEM, VMEM, VMEM, VMEM, ANY, ANY, VMEM, VMEM, VMEM, ANY, ANY, ANY],
        out_specs=(ANY,) * 4,
        scratch_shapes=[
            pltpu.VMEM((n_t, rows, width), bf16),
            pltpu.VMEM(w.shape, bf16),
            pltpu.VMEM(wt.shape, bf16),
            pltpu.VMEM((n_p, keys, cols), bf16),
            pltpu.VMEM((n_p, keys, cols), bf16),
            pltpu.VMEM((n_p * trows, cols), bf16),
            pltpu.VMEM((n_p * trows, cols), bf16),
            pltpu.VMEM((keys, cols), bf16),
            pltpu.VMEM((keys, cols), f32),
            pltpu.VMEM((keys, cols), f32),
            pltpu.VMEM((keys, cols), f32),
            pltpu.VMEM((n_t, rows, cols), bf16),
            dma((2,)),
            dma((2, n_p, 2)),
            dma((2, n_p, 2)),
            dma((2, n_t, 3)),
            dma((n_t, 3)),
            dma((n_p, 2)),
            dma((n_p, 2)),
            dma((n_t, 2, n_p)),
            dma((n_t, 2, n_p)),
            dma((n_t, 2)),
            dma((n_t, 2)),
            dma((3,)),
        ],
        compiler_params=pltpu.CompilerParams(
            collective_id=0, has_side_effects=True, vmem_limit_bytes=63 * 1024 * 1024
        ),
        name="fused",
    )(x, ishift[None, :], iscale[None, :], text, tshift[None, :], tscale[None, :], w, wt, q_gain[None, :], k_gain[None, :], t_gain[None, :],
      out_weight, stale_k, stale_v)


def finish_kernel(n_t, x_ref, nk_ref, nv_ref, ow_ref, t_ref, g_ref, *refs):
    t = lax.axis_index("tensor")
    walls, (o_ref, ko_ref, vo_ref) = refs[: n_t - 1], refs[n_t - 1 :]
    total = jnp.dot(x_ref[t], ow_ref[...], preferred_element_type=jnp.float32)
    for j in range(1, n_t):
        total = total + jnp.dot(x_ref[lax.rem(t + j, n_t)], walls[j - 1][0], preferred_element_type=jnp.float32)
    o_ref[...] = (t_ref[...].astype(jnp.float32) + g_ref[...] * total).astype(jnp.bfloat16)
    ko_ref[...] = nk_ref[...]
    vo_ref[...] = nv_ref[...]


def finish(att, wall, out_weight, tokens, gate, new_k, new_v):
    n_t, rows, depth = att.shape
    width = tokens.shape[1]
    keys, cols = new_k.shape
    steps = 6 if width % 6 == 0 and (width // 6) % 128 == 0 and keys % 96 == 0 else 4
    tile = width // steps
    part = pl.BlockSpec((keys // steps, cols), lambda j: (j, 0))

    def other(i):
        def index(j):
            return (lax.rem(lax.axis_index("tensor") + i, n_t), 0, j)

        return pl.BlockSpec((1, depth, tile), index)

    return pl.pallas_call(
        functools.partial(finish_kernel, n_t),
        grid=(steps,),
        out_shape=(
            jax.ShapeDtypeStruct(tokens.shape, jnp.bfloat16),
            jax.ShapeDtypeStruct(new_k.shape, jnp.bfloat16),
            jax.ShapeDtypeStruct(new_v.shape, jnp.bfloat16),
        ),
        in_specs=[
            pl.BlockSpec((n_t, rows, depth), lambda j: (0, 0, 0)),
            part,
            part,
            pl.BlockSpec((depth, tile), lambda j: (0, j)),
            pl.BlockSpec((rows, tile), lambda j: (0, j)),
            pl.BlockSpec((1, tile), lambda j: (0, j)),
        ]
        + [other(i) for i in range(1, n_t)],
        out_specs=(pl.BlockSpec((rows, tile), lambda j: (0, j)), part, part),
        name="finish",
    )(att, new_k, new_v, out_weight, tokens, gate[None, :], *[wall] * (n_t - 1))


def per_device(
    n_patch,
    n_tensor,
    tokens,
    text_tokens,
    img_shift,
    img_scale,
    img_gate,
    txt_shift,
    txt_scale,
    qkv_weight,
    txt_kv_weight,
    q_gain,
    k_gain,
    txt_k_gain,
    out_weight,
    stale_keys,
    stale_values,
):
    new_keys, new_values, att, wall = fused(
        n_patch, n_tensor, tokens, img_shift, img_scale, text_tokens, txt_shift, txt_scale,
        jnp.transpose(qkv_weight, (1, 0, 2)), txt_kv_weight,
        q_gain, k_gain, txt_k_gain, out_weight, stale_keys, stale_values,
    )
    wall = wall.reshape(n_tensor, -1, wall.shape[-1])
    return finish(att, wall, out_weight, tokens, img_gate, new_keys, new_values)


def solution(mesh):
    placed = (
        P(("patch", "tensor"), None),
        P("patch", None),
        P(),
        P(),
        P(),
        P(),
        P(),
        P(None, None, "tensor"),
        P(None, None, "tensor"),
        P(),
        P(),
        P(),
        P("tensor", None),
        P("patch", "tensor"),
        P("patch", "tensor"),
    )
    return jax.shard_map(
        functools.partial(per_device, mesh.shape["patch"], mesh.shape["tensor"]),
        mesh=mesh,
        in_specs=placed,
        out_specs=(P(("patch", "tensor"), None), P("patch", "tensor"), P("patch", "tensor")),
        check_vma=False,
    )
```
